8 devices in a mesh: rep: 2 (over y, z), dp: 4 (over x, core).
Axes of the slice: x: 2, y: 2, z: 1, core: 2. Of those that a mesh axis runs over, the one named last changes fastest.
Arguments:
- x: bfloat16 [8, 2048, 1024], P(('rep', 'dp')), parts along dimension 0
- dy: bfloat16 [8, 2048, 1024], P(('rep', 'dp')), parts along dimension 0
- w_gate: bfloat16 [2, 1024, 6144], replicated
- w_up: bfloat16 [2, 1024, 6144], replicated
- w_down: bfloat16 [2, 6144, 1024], replicated
- m_w_gate: float32 [2, 1024, 6144], P(None, 'dp')
- m_w_up: float32 [2, 1024, 6144], P(None, 'dp')
- m_w_down: float32 [2, 6144, 1024], P(None, 'dp')
- v_w_gate: float32 [2, 1024, 6144], P(None, 'dp')
- v_w_up: float32 [2, 1024, 6144], P(None, 'dp')
- v_w_down: float32 [2, 6144, 1024], P(None, 'dp')
Outputs:
- output 1: bfloat16 [4, 1024, 6144], P('rep'), parts along dimension 0
- output 2: bfloat16 [4, 1024, 6144], P('rep'), parts along dimension 0
- output 3: bfloat16 [4, 6144, 1024], P('rep'), parts along dimension 0
- output 4: float32 [4, 1024, 6144], P('rep', 'dp'), parts along dimension 0
- output 5: float32 [4, 1024, 6144], P('rep', 'dp'), parts along dimension 0
- output 6: float32 [4, 6144, 1024], P('rep', 'dp'), parts along dimension 0
- output 7: float32 [4, 1024, 6144], P('rep', 'dp'), parts along dimension 0
- output 8: float32 [4, 1024, 6144], P('rep', 'dp'), parts along dimension 0
- output 9: float32 [4, 6144, 1024], P('rep', 'dp'), parts along dimension 0
There are 2 independent parts. The reference program is written for one: setup_inputs(seed, part) draws one part's arguments, and reference() takes and returns one part's arrays. A program takes and returns all parts, laid end to end along the dimension named above; an argument that names none is the same for every part.
All inputs are finite; a program needn't handle non-finite values.
Results may differ from the reference program's by a relative error of at most 0.022.
Values are sent between devices in bfloat16 or wider.
A program may use at most 2 GiB of HBM per device.

```python
import jax
import jax.numpy as jnp
from jax import lax

SEQUENCES = 4
TOKENS = 2048
D = 1024
FF = 6144
LAYERS = 2
NAMES = ("w_gate", "w_up", "w_down")
SHAPES = {"w_gate": (LAYERS, D, FF), "w_up": (LAYERS, D, FF), "w_down": (LAYERS, FF, D)}


def bump(key, n, height):
    away = (jnp.arange(n, dtype=jnp.int32) - jax.random.randint(key, (), 0, n, jnp.int32)) % n
    return jnp.where(away < n // 8, height, 1.0)


def together(key, own, strength):
    shared = jax.random.normal(key, own.shape[1:], jnp.float32)
    return (own + strength * shared) * lax.rsqrt(1 + strength * strength)


def setup_inputs(seed: int = 0, part: int = 0) -> dict:
    kx, kdy, ka, kb, kz, kf, kh, kl, *keys = jax.random.split(jax.random.key(seed), 8 + 3 * len(NAMES))
    kx, kdy, ka, kb = (jax.random.fold_in(k, part) for k in (kx, kdy, ka, kb))
    kw, km, kv = (keys[i::3] for i in range(3))
    shape = (SEQUENCES, TOKENS, D)
    much_x, much_dy = jax.random.uniform(kz, (2,), jnp.float32, 0.0, 1.0)
    loud = 2.0 ** jax.random.uniform(jax.random.fold_in(kz, 1), (), jnp.float32, -1.0, 2.0)
    layers = 2.0 ** jax.random.uniform(kl, (LAYERS, 1, 1), jnp.float32, -1.0, 1.0)
    x = together(ka, jax.random.normal(kx, shape, jnp.float32), much_x) * bump(kf, D, 4.0)
    dy = together(kb, jax.random.normal(kdy, shape, jnp.float32), much_dy)
    drawn = {"x": x.astype(jnp.bfloat16), "dy": (loud * dy * (SEQUENCES * TOKENS) ** -0.5).astype(jnp.bfloat16)}
    for key, name in zip(kw, NAMES, strict=True):
        w = jax.random.normal(key, SHAPES[name], jnp.float32) * SHAPES[name][1] ** -0.5
        drawn[name] = (w * {"w_gate": 1.0, "w_up": bump(kh, FF, 4.0), "w_down": layers}[name]).astype(jnp.bfloat16)
    for key, name in zip(km, NAMES, strict=True):
        drawn[f"m_{name}"] = 0.1 * jax.random.normal(key, SHAPES[name], jnp.float32)
    for key, name in zip(kv, NAMES, strict=True):
        drawn[f"v_{name}"] = jax.random.uniform(key, SHAPES[name], jnp.float32, 0.005, 0.015)
    return drawn


def matmul(a, w):
    return jnp.dot(a, w, preferred_element_type=jnp.float32).astype(jnp.bfloat16)


def normed(h):
    wide = h.astype(jnp.float32)
    scale = lax.rsqrt(jnp.mean(wide**2, -1, keepdims=True) + 1e-6)
    return (wide * scale).astype(jnp.bfloat16)


def layer(h, w):
    a = normed(h)
    gate = jnp.dot(a, w["w_gate"], preferred_element_type=jnp.float32)
    up = jnp.dot(a, w["w_up"], preferred_element_type=jnp.float32)
    return h + matmul((jax.nn.silu(gate) * up).astype(jnp.bfloat16), w["w_down"])


def adamw(w, m, v, g):
    m = 0.9 * m + 0.1 * g
    v = 0.95 * v + 0.05 * g * g
    step = m * lax.rsqrt(v + 1e-8) + 0.1 * w
    return (w - 0.02 * step).astype(jnp.bfloat16), m, v


def clipped(gradients, sum_of_squares, count):
    factor = jnp.minimum(1.0, 0.5 * lax.rsqrt(sum_of_squares / count + 1e-30))
    return [g * factor for g in gradients]


def stack(weights, h):
    return lax.scan(lambda h, w: (layer(h, w), None), h, weights)[0]


def reference(x, dy, w_gate, w_up, w_down, m_w_gate, m_w_up, m_w_down, v_w_gate, v_w_up, v_w_down):
    weights = dict(zip(NAMES, (w_gate, w_up, w_down), strict=True))

    def take(so_far, sequence):
        h, by_y = sequence
        _, back = jax.vjp(lambda w: stack(w, h), weights)
        return jax.tree.map(lambda total, term: total + term.astype(jnp.float32), so_far, back(by_y)[0]), None

    none_yet = {name: jnp.zeros(w.shape, jnp.float32) for name, w in weights.items()}
    by_weights, _ = lax.scan(take, none_yet, (x, dy))
    gradients = [by_weights[name].astype(jnp.bfloat16).astype(jnp.float32) for name in NAMES]
    gradients = clipped(gradients, sum(jnp.sum(g * g) for g in gradients), sum(g.size for g in gradients))
    new = [
        adamw(w.astype(jnp.float32), m, v, g)
        for w, m, v, g in zip((w_gate, w_up, w_down), (m_w_gate, m_w_up, m_w_down), (v_w_gate, v_w_up, v_w_down), gradients, strict=True)
    ]
    return tuple(one[which] for which in range(3) for one in new)
```

```python
import functools

import jax
import jax.numpy as jnp
from jax import lax
from jax.experimental import pallas as pl
from jax.experimental.pallas import tpu as pltpu
from jax.sharding import PartitionSpec as P

F32, BF16 = jnp.float32, jnp.bfloat16
LAYERS = 2
T, D, F = 2048, 1024, 6144
QD, QF = D // 4, F // 4
LANES = 128
TILE = 2 * LANES
TILES = F // TILE
ROWS = 256
LAG = 3
OUT_SLOTS, FAR_SLOTS = LAG + 2, 2 * LAG
CROSS = [(i, i ^ 2) for i in range(4)]
PAIR = [(i, i ^ 1) for i in range(4)]
VMEM_LIMIT = 64 * 1024 * 1024 - 65536


def dot(a, b, contract):
    return lax.dot_general(a, b, ((contract[:1], contract[1:]), ((), ())), preferred_element_type=F32)


def norm_scale(wide):
    return lax.rsqrt(jnp.mean(wide * wide, -1, keepdims=True) + 1e-6)


def hidden_tile(t):
    first = (t % 2) * (2 * QF) + (t // 2) * LANES
    return first, first + QF


def gradients_kernel(
    x_hbm, dy_hbm, wg_hbm, wu_hbm, wd_hbm,
    gg_hbm, gu_hbm, gd_hbm, ss_out, sr_hbm, hid_hbm,
    h, a, a0, dy, acc, w, wd, sr, hid, dgu,
    out_gu, out_d, near_gu, near_d, send_gu, send_d, far_gu, far_d, g_gu, g_d, ss, ss_all,
    in_sem, w_sem, save_sem, near_send, near_recv, far_send, far_recv, g_sem, ss_send, ss_recv,
):
    me, rep = lax.axis_index("dp"), lax.axis_index("rep")
    chip, core = me // 2, me % 2
    partner = chip * 2 + (1 - core)
    across = (1 - chip) * 2 + core

    def copy(src, dst, sem):
        return pltpu.make_async_copy(src, dst, sem)

    def remote(src, dst, send, recv, to):
        return pltpu.make_async_remote_copy(
            src, dst, send, recv, device_id=(rep, to), device_id_type=pl.DeviceIdType.MESH
        )

    def weight_copies(layer, t, slot, gate_up=True):
        copies = []
        for i, first in enumerate(hidden_tile(t)):
            first = pl.multiple_of(first, LANES)
            copies.append(copy(wd_hbm.at[layer, pl.ds(first, LANES)], wd.at[slot, pl.ds(i * LANES, LANES)], w_sem.at[slot, i]))
            if gate_up:
                for j, whole in enumerate((wg_hbm, wu_hbm)):
                    to = w.at[slot, :, pl.ds(j * TILE + i * LANES, LANES)]
                    copies.append(copy(whole.at[layer, :, pl.ds(first, LANES)], to, w_sem.at[slot, 2 + 2 * j + i]))
        return copies

    def start(copies):
        for c in copies:
            c.start()

    def wait(copies):
        for c in copies:
            c.wait()

    def save_copies(t, slot):
        return [copy(sr.at[slot], sr_hbm.at[t], save_sem.at[slot, 0]), copy(hid.at[slot], hid_hbm.at[t], save_sem.at[slot, 1])]

    def load_copies(t, slot):
        return [copy(sr_hbm.at[t], sr.at[slot], save_sem.at[slot, 0]), copy(hid_hbm.at[t], hid.at[slot], save_sem.at[slot, 1])]

    def near_copies(g):
        slot = g % OUT_SLOTS
        return [
            remote(out_gu.at[slot, :, 1 - core], near_gu.at[slot], near_send.at[slot, 0], near_recv.at[slot, 0], partner),
            remote(out_d.at[slot, 1 - core], near_d.at[slot], near_send.at[slot, 1], near_recv.at[slot, 1], partner),
        ]

    def far_gu_copy(g):
        slot = g % FAR_SLOTS
        return remote(send_gu.at[slot], far_gu.at[slot], far_send.at[slot, 0], far_recv.at[slot, 0], across)

    def far_d_copy(g):
        slot = g % FAR_SLOTS
        return remote(send_d.at[slot], far_d.at[slot], far_send.at[slot, 1], far_recv.at[slot, 1], across)

    def send_across(g):
        slot, far = g % OUT_SLOTS, g % FAR_SLOTS
        wait(near_copies(g))
        send_gu[far] = (out_gu[slot, 1 - chip, core].astype(F32) + near_gu[slot, 1 - chip].astype(F32)).astype(BF16)
        far_gu_copy(g).start()

        @pl.when(g % 2 != chip)
        def _():
            send_d[far] = (out_d[slot, core].astype(F32) + near_d[slot].astype(F32)).astype(BF16)
            far_d_copy(g).start()

    def gu_copies(g):
        layer, t, slot = 1 - g // TILES, g % TILES, g % 2
        copies = []
        for i, first in enumerate(hidden_tile(t)):
            first = pl.multiple_of(first, LANES)
            for j, to in enumerate((gg_hbm, gu_hbm)):
                src = g_gu.at[slot, :, pl.ds(j * TILE + i * LANES, LANES)]
                copies.append(copy(src, to.at[layer, :, pl.ds(first, LANES)], g_sem.at[slot, 2 * j + i]))
        return copies

    def d_copy(g):
        layer, t, slot = 1 - g // TILES, g % TILES, (g // 2) % 2
        return copy(g_d.at[slot], gd_hbm.at[layer, pl.ds(pl.multiple_of((t // 2) * LANES, LANES), LANES)], g_sem.at[slot, 4])

    def add_squares(block):
        wide = block.astype(F32)
        wide = jnp.sum((wide * wide).reshape(-1, 8, wide.shape[1]), 0)
        ss[...] += sum(wide[:, i : i + LANES] for i in range(0, wide.shape[1], LANES))

    def collect(g):
        slot, far = g % OUT_SLOTS, g % FAR_SLOTS
        far_gu_copy(g).wait()

        @pl.when(g >= 2)
        def _():
            wait(gu_copies(g - 2))

        total = out_gu[slot, chip, core].astype(F32) + near_gu[slot, chip].astype(F32) + far_gu[far].astype(F32)
        g_gu[g % 2] = total.astype(BF16)
        start(gu_copies(g))
        add_squares(total.astype(BF16))

        @pl.when(g % 2 != chip)
        def _():
            far_d_copy(g).wait_send()

        @pl.when(g % 2 == chip)
        def _():
            far_d_copy(g).wait_recv()

            @pl.when(g >= 4)
            def _():
                d_copy(g - 4).wait()

            total = out_d[slot, core].astype(F32) + near_d[slot].astype(F32) + far_d[far].astype(F32)
            g_d[(g // 2) % 2] = total.astype(BF16)
            d_copy(g).start()
            add_squares(total.astype(BF16))

    start(weight_copies(0, 0, 0))
    start([copy(x_hbm, h, in_sem.at[0]), copy(dy_hbm, dy, in_sem.at[1])])
    barrier = pltpu.get_barrier_semaphore()
    for other in range(1, 4):
        pl.semaphore_signal(barrier, inc=1, device_id=(rep, lax.rem(me + other, 4)), device_id_type=pl.DeviceIdType.MESH)
    pl.semaphore_wait(barrier, 3)
    ss[...] = jnp.zeros_like(ss)
    copy(x_hbm, h, in_sem.at[0]).wait()

    for r in range(0, T, ROWS):
        rows = pl.ds(r, ROWS)
        wide = h[rows].astype(F32)
        a0[rows] = (wide * norm_scale(wide)).astype(BF16)
        acc[rows] = jnp.zeros((ROWS, D), F32)

    def forward(t, _):
        slot = t % 2
        wait(weight_copies(0, t, slot))

        @pl.when(t + 1 < TILES)
        def _():
            start(weight_copies(0, t + 1, 1 - slot))

        @pl.when(t >= 2)
        def _():
            wait(save_copies(t - 2, slot))

        for r in range(0, T, ROWS):
            rows = pl.ds(r, ROWS)
            both = dot(a0[rows], w[slot], (1, 0))
            gate, up = both[:, :TILE], both[:, TILE:]
            s = jax.nn.sigmoid(gate)
            silu = gate * s
            sr[slot, rows, :TILE] = up * (s + silu * (1.0 - s))
            sr[slot, rows, TILE:] = silu
            hidden = (silu * up).astype(BF16)
            hid[slot, rows] = hidden
            acc[rows] += dot(hidden, wd[slot], (1, 0))
        start(save_copies(t, slot))
        return 0

    lax.fori_loop(0, TILES, forward, 0)
    start(weight_copies(1, 0, 0))
    copy(dy_hbm, dy, in_sem.at[1]).wait()
    for r in range(0, T, ROWS):
        rows = pl.ds(r, ROWS)
        state = h[rows] + acc[rows].astype(BF16)
        h[rows] = state
        wide = state.astype(F32)
        a[rows] = (wide * norm_scale(wide)).astype(BF16)
        acc[rows] = jnp.zeros((ROWS, D), F32)
    wait(save_copies(TILES - 2, 0))
    wait(save_copies(TILES - 1, 1))

    def products(g, states, hidden):
        slot = g % OUT_SLOTS
        down = dot(hidden, dy[...], (0, 0)).astype(BF16)
        for i in range(2):
            out_d[slot, i] = down[i * LANES : (i + 1) * LANES]
        both = dot(states[...], dgu[...], (0, 0)).astype(BF16)
        for q in range(4):
            out_gu[slot, q // 2, q % 2] = both[q * QD : (q + 1) * QD]
        start(near_copies(g))

    def second(g, _):
        slot = g % 2
        wait(weight_copies(1, g, slot))

        @pl.when(g + 1 < TILES)
        def _():
            start(weight_copies(1, g + 1, 1 - slot))

        for r in range(0, T, ROWS):
            rows = pl.ds(r, ROWS)
            both = dot(a[rows], w[slot], (1, 0))
            gate, up = both[:, :TILE], both[:, TILE:]
            by_hidden = dot(dy[rows], wd[slot], (1, 1)).astype(BF16).astype(F32)
            s = jax.nn.sigmoid(gate)
            silu = gate * s
            hid[0, rows] = (silu * up).astype(BF16)
            dgu[rows, :TILE] = (by_hidden * (up * (s + silu * (1.0 - s)))).astype(BF16)
            dgu[rows, TILE:] = (by_hidden * silu).astype(BF16)

        @pl.when(g >= 1)
        def _():
            send_across(g - 1)

        products(g, a, hid[0])
        for r in range(0, T, ROWS):
            rows = pl.ds(r, ROWS)
            acc[rows] += dot(dgu[rows], w[slot], (1, 1))

        @pl.when(g >= LAG)
        def _():
            collect(g - LAG)

        return 0

    lax.fori_loop(0, TILES, second, 0)
    start(weight_copies(0, 0, 0, False))
    start(load_copies(0, 0))
    for r in range(0, T, ROWS):
        rows = pl.ds(r, ROWS)
        wide = h[rows].astype(F32)
        scale = norm_scale(wide)
        by_a = acc[rows].astype(BF16).astype(F32)
        along = jnp.mean(by_a * wide, -1, keepdims=True)
        dy[rows] += (by_a * scale - wide * (scale * scale * scale * along)).astype(BF16)

    def first(t, _):
        g, slot = t + TILES, t % 2
        wait(weight_copies(0, t, slot, False))
        wait(load_copies(t, slot))

        @pl.when(t + 1 < TILES)
        def _():
            start(weight_copies(0, t + 1, 1 - slot, False))
            start(load_copies(t + 1, 1 - slot))

        for r in range(0, T, ROWS):
            rows = pl.ds(r, ROWS)
            by_hidden = dot(dy[rows], wd[slot], (1, 1)).astype(BF16).astype(F32)
            dgu[rows, :TILE] = (by_hidden * sr[slot, rows, :TILE]).astype(BF16)
            dgu[rows, TILE:] = (by_hidden * sr[slot, rows, TILE:]).astype(BF16)
        send_across(g - 1)
        products(g, a0, hid[slot])
        collect(g - LAG)
        return 0

    lax.fori_loop(0, TILES, first, 0)
    last = LAYERS * TILES
    send_across(last - 1)
    for g in range(last - LAG, last):
        collect(g)
    wait(gu_copies(last - 2) + gu_copies(last - 1))
    d_copy(last - 4 + chip).wait()
    d_copy(last - 2 + chip).wait()

    ss_all[me] = ss[...]
    sums = [
        remote(ss, ss_all.at[me], ss_send.at[i], ss_recv.at[me], lax.rem(me + 1 + i, 4)) for i in range(3)
    ]
    start(sums)
    for i in range(3):
        frm = lax.rem(me + 1 + i, 4)
        remote(ss, ss_all.at[frm], ss_send.at[i], ss_recv.at[frm], frm).wait()
    ss_out[...] = ss_all[0] + ss_all[1] + ss_all[2] + ss_all[3]


def gradients(x, dy, wg, wu, wd):
    hbm = pl.BlockSpec(memory_space=pl.ANY)
    vmem = pl.BlockSpec(memory_space=pltpu.VMEM)
    shape = jax.ShapeDtypeStruct
    tokens = pltpu.VMEM((T, D), BF16)
    dma = pltpu.SemaphoreType.DMA
    return pl.pallas_call(
        gradients_kernel,
        name="gradients",
        in_specs=[hbm] * 5,
        out_specs=[hbm] * 3 + [vmem] + [hbm] * 2,
        out_shape=[
            shape((LAYERS, QD, F), BF16),
            shape((LAYERS, QD, F), BF16),
            shape((LAYERS, QF, D), BF16),
            shape((8, LANES), F32),
            shape((TILES, T, 2 * TILE), F32),
            shape((TILES, T, TILE), BF16),
        ],
        scratch_shapes=[
            tokens, tokens, tokens, tokens,
            pltpu.VMEM((T, D), F32),
            pltpu.VMEM((2, D, 2 * TILE), BF16),
            pltpu.VMEM((2, TILE, D), BF16),
            pltpu.VMEM((2, T, 2 * TILE), F32),
            pltpu.VMEM((2, T, TILE), BF16),
            pltpu.VMEM((T, 2 * TILE), BF16),
            pltpu.VMEM((OUT_SLOTS, 2, 2, QD, 2 * TILE), BF16),
            pltpu.VMEM((OUT_SLOTS, 2, LANES, D), BF16),
            pltpu.VMEM((OUT_SLOTS, 2, QD, 2 * TILE), BF16),
            pltpu.VMEM((OUT_SLOTS, LANES, D), BF16),
            pltpu.VMEM((FAR_SLOTS, QD, 2 * TILE), BF16),
            pltpu.VMEM((FAR_SLOTS, LANES, D), BF16),
            pltpu.VMEM((FAR_SLOTS, QD, 2 * TILE), BF16),
            pltpu.VMEM((FAR_SLOTS, LANES, D), BF16),
            pltpu.VMEM((2, QD, 2 * TILE), BF16),
            pltpu.VMEM((2, LANES, D), BF16),
            pltpu.VMEM((8, LANES), F32),
            pltpu.VMEM((4, 8, LANES), F32),
            dma((2,)), dma((2, 6)), dma((2, 2)),
            dma((OUT_SLOTS, 2)), dma((OUT_SLOTS, 2)), dma((FAR_SLOTS, 2)), dma((FAR_SLOTS, 2)),
            dma((2, 5)), dma((3,)), dma((4,)),
        ],
        compiler_params=pltpu.CompilerParams(collective_id=0, has_side_effects=True, vmem_limit_bytes=VMEM_LIMIT),
        cost_estimate=pl.CostEstimate(flops=15 * 2 * T * D * F, bytes_accessed=500_000_000, transcendentals=4 * T * F),
    )(x, dy, wg, wu, wd)


def gathered(out, block, layer, me):
    n = block.shape[0]
    far = lax.ppermute(block, "dp", CROSS)
    for part, q in (
        (block, me),
        (lax.ppermute(block, "dp", PAIR), me ^ 1),
        (far, me ^ 2),
        (lax.ppermute(far, "dp", PAIR), me ^ 3),
    ):
        out = lax.dynamic_update_slice(out, part[None], (layer, q * n, 0))
    return out


def step(x, dy, wg, wu, wd, *moments):
    me = lax.axis_index("dp")
    m, v = moments[:3], moments[3:]
    *grads, squares = gradients(x[0], dy[0], wg, wu, wd)[:4]
    count = LAYERS * 3 * D * F
    factor = jnp.minimum(1.0, 0.5 * lax.rsqrt(jnp.sum(squares) / count + 1e-30))

    outs = ([], [], [])
    for i, (grad, w) in enumerate(zip(grads, (wg, wu, wd), strict=True)):
        n = w.shape[1] // 4
        out = jnp.zeros(w.shape, BF16)
        old = lax.dynamic_slice_in_dim(w, me * n, n, 1).astype(F32)
        grad = grad.astype(F32) * factor
        new_m = 0.9 * m[i] + 0.1 * grad
        new_v = 0.95 * v[i] + 0.05 * grad * grad
        new_w = (old - 0.02 * (new_m * lax.rsqrt(new_v + 1e-8) + 0.1 * old)).astype(BF16)
        for layer in range(LAYERS):
            out = gathered(out, new_w[layer], layer, me)
        for to, value in zip(outs, (out, new_m, new_v), strict=True):
            to.append(value)
    return tuple(outs[0] + outs[1] + outs[2])


def solution(mesh):
    tokens = P(("rep", "dp"), None, None)
    whole, rows = P(None, None, None), P(None, "dp", None)
    return jax.shard_map(
        step,
        mesh=mesh,
        in_specs=(tokens,) * 2 + (whole,) * 3 + (rows,) * 6,
        out_specs=(P("rep", None, None),) * 3 + (P("rep", "dp", None),) * 6,
        check_vma=False,
    )
```

```python
import functools

import jax
import jax.numpy as jnp
from jax import lax
from jax.experimental import pallas as pl
from jax.experimental.pallas import tpu as pltpu
from jax.sharding import PartitionSpec as P

F32, BF16 = jnp.float32, jnp.bfloat16
LAYERS = 2
T, D, F = 2048, 1024, 6144
QD, QF = D // 4, F // 4
LANES = 128
TILE = 2 * LANES
TILES = F // TILE
ROWS = 256
LAG = 3
OUT_SLOTS, FAR_SLOTS = LAG + 2, 2 * LAG
CROSS = [(i, i ^ 2) for i in range(4)]
PAIR = [(i, i ^ 1) for i in range(4)]
VMEM_LIMIT = 64 * 1024 * 1024 - 65536


def dot(a, b, contract):
    return lax.dot_general(a, b, ((contract[:1], contract[1:]), ((), ())), preferred_element_type=F32)


def norm_scale(wide):
    return lax.rsqrt(jnp.mean(wide * wide, -1, keepdims=True) + 1e-6)


def hidden_tile(t):
    first = (t % 2) * (2 * QF) + (t // 2) * LANES
    return first, first + QF


def gradients_kernel(
    x_hbm, dy_hbm, wg_hbm, wu_hbm, wd_hbm,
    gg_hbm, gu_hbm, gd_hbm, ss_out, sr_hbm, hid_hbm,
    h, a, a0, dy, acc, w, wd, sr, hid, dgu,
    out_gu, out_d, near_gu, near_d, send_gu, send_d, far_gu, far_d, g_gu, g_d, ss, ss_all,
    in_sem, w_sem, save_sem, near_send, near_recv, far_send, far_recv, g_sem, ss_send, ss_recv,
):
    me, rep = lax.axis_index("dp"), lax.axis_index("rep")
    chip, core = me // 2, me % 2
    partner = chip * 2 + (1 - core)
    across = (1 - chip) * 2 + core

    def copy(src, dst, sem):
        return pltpu.make_async_copy(src, dst, sem)

    def remote(src, dst, send, recv, to):
        return pltpu.make_async_remote_copy(
            src, dst, send, recv, device_id=(rep, to), device_id_type=pl.DeviceIdType.MESH
        )

    def down_copies(layer, t, slot):
        copies = []
        for i, first in enumerate(hidden_tile(t)):
            to = wd.at[pl.ds(pl.multiple_of(slot * TILE + i * LANES, LANES), LANES)]
            copies.append(copy(wd_hbm.at[layer, pl.ds(pl.multiple_of(first, LANES), LANES)], to, w_sem.at[slot, i]))
        return copies

    def gate_up_copies(layer, t, slot):
        copies = []
        for i, first in enumerate(hidden_tile(t)):
            for j, whole in enumerate((wg_hbm, wu_hbm)):
                to = w.at[slot, :, pl.ds(j * TILE + i * LANES, LANES)]
                src = whole.at[layer, :, pl.ds(pl.multiple_of(first, LANES), LANES)]
                copies.append(copy(src, to, w_sem.at[slot, 2 + 2 * j + i]))
        return copies

    def weight_copies(layer, t, slot, gate_up=True):
        return down_copies(layer, t, slot) + (gate_up_copies(layer, t, slot) if gate_up else [])

    def start(copies):
        for c in copies:
            c.start()

    def wait(copies):
        for c in copies:
            c.wait()

    def save_copies(t, slot):
        return [copy(sr.at[slot], sr_hbm.at[t], save_sem.at[slot, 0]), copy(hid.at[slot], hid_hbm.at[t], save_sem.at[slot, 1])]

    def load_copies(t, slot):
        return [copy(sr_hbm.at[t], sr.at[slot], save_sem.at[slot, 0]), copy(hid_hbm.at[t], hid.at[slot], save_sem.at[slot, 1])]

    def near_copies(g):
        slot = g % OUT_SLOTS
        return [
            remote(out_gu.at[slot, :, 1 - core], near_gu.at[slot], near_send.at[slot, 0], near_recv.at[slot, 0], partner),
            remote(out_d.at[slot, 1 - core], near_d.at[slot], near_send.at[slot, 1], near_recv.at[slot, 1], partner),
        ]

    def far_gu_copy(g):
        slot = g % FAR_SLOTS
        return remote(send_gu.at[slot], far_gu.at[slot], far_send.at[slot, 0], far_recv.at[slot, 0], across)

    def far_d_copy(g):
        slot = g % FAR_SLOTS
        return remote(send_d.at[slot], far_d.at[slot], far_send.at[slot, 1], far_recv.at[slot, 1], across)

    def send_across(g):
        slot, far = g % OUT_SLOTS, g % FAR_SLOTS
        wait(near_copies(g))
        send_gu[far] = (out_gu[slot, 1 - chip, core].astype(F32) + near_gu[slot, 1 - chip].astype(F32)).astype(BF16)
        far_gu_copy(g).start()

        @pl.when(g % 2 != chip)
        def _():
            send_d[far] = (out_d[slot, core].astype(F32) + near_d[slot].astype(F32)).astype(BF16)
            far_d_copy(g).start()

    def gu_copies(g):
        layer, t, slot = 1 - g // TILES, g % TILES, g % 2
        copies = []
        for i, first in enumerate(hidden_tile(t)):
            first = pl.multiple_of(first, LANES)
            for j, to in enumerate((gg_hbm, gu_hbm)):
                src = g_gu.at[slot, :, pl.ds(j * TILE + i * LANES, LANES)]
                copies.append(copy(src, to.at[layer, :, pl.ds(first, LANES)], g_sem.at[slot, 2 * j + i]))
        return copies

    def d_copy(g):
        layer, t, slot = 1 - g // TILES, g % TILES, (g // 2) % 2
        return copy(g_d.at[slot], gd_hbm.at[layer, pl.ds(pl.multiple_of((t // 2) * LANES, LANES), LANES)], g_sem.at[slot, 4])

    def add_squares(block):
        wide = block.astype(F32)
        wide = jnp.sum((wide * wide).reshape(-1, 8, wide.shape[1]), 0)
        ss[...] += sum(wide[:, i : i + LANES] for i in range(0, wide.shape[1], LANES))

    def collect(g):
        slot, far = g % OUT_SLOTS, g % FAR_SLOTS
        far_gu_copy(g).wait()

        @pl.when(g >= 2)
        def _():
            wait(gu_copies(g - 2))

        total = out_gu[slot, chip, core].astype(F32) + near_gu[slot, chip].astype(F32) + far_gu[far].astype(F32)
        g_gu[g % 2] = total.astype(BF16)
        start(gu_copies(g))
        add_squares(total.astype(BF16))

        @pl.when(g % 2 != chip)
        def _():
            far_d_copy(g).wait_send()

        @pl.when(g % 2 == chip)
        def _():
            far_d_copy(g).wait_recv()

            @pl.when(g >= 4)
            def _():
                d_copy(g - 4).wait()

            total = out_d[slot, core].astype(F32) + near_d[slot].astype(F32) + far_d[far].astype(F32)
            g_d[(g // 2) % 2] = total.astype(BF16)
            d_copy(g).start()
            add_squares(total.astype(BF16))

    for slot in range(2):
        start(weight_copies(0, slot, slot))
    start([copy(x_hbm, h, in_sem.at[0]), copy(dy_hbm, dy, in_sem.at[1])])
    barrier = pltpu.get_barrier_semaphore()
    for other in range(1, 4):
        pl.semaphore_signal(barrier, inc=1, device_id=(rep, lax.rem(me + other, 4)), device_id_type=pl.DeviceIdType.MESH)
    pl.semaphore_wait(barrier, 3)
    ss[...] = jnp.zeros_like(ss)
    acc[...] = jnp.zeros_like(acc)
    copy(x_hbm, h, in_sem.at[0]).wait()

    for r in range(0, T, ROWS):
        rows = pl.ds(r, ROWS)
        wide = h[rows].astype(F32)
        a0[rows] = (wide * norm_scale(wide)).astype(BF16)

    def forward(p, _):
        for slot in range(2):
            t = 2 * p + slot
            wait(gate_up_copies(0, t, slot))

            @pl.when(p >= 1)
            def _():
                wait(save_copies(t - 2, slot))

            for r in range(0, T, ROWS):
                rows = pl.ds(r, ROWS)
                both = dot(a0[rows], w[slot], (1, 0))
                gate, up = both[:, :TILE], both[:, TILE:]
                s = jax.nn.sigmoid(gate)
                silu = gate * s
                sr[slot, rows, :TILE] = up * (s + silu * (1.0 - s))
                sr[slot, rows, TILE:] = silu
                hidden = (silu * up).astype(BF16)
                hid[slot, rows] = hidden
                dgu[rows, slot * TILE : (slot + 1) * TILE] = hidden
            start(save_copies(t, slot))

            @pl.when(p + 1 < TILES // 2)
            def _():
                start(gate_up_copies(0, t + 2, slot))

        for slot in range(2):
            wait(down_copies(0, 2 * p + slot, slot))
        for r in range(0, T, ROWS):
            rows = pl.ds(r, ROWS)
            acc[rows] += dot(dgu[rows], wd[...], (1, 0))

        @pl.when(p + 1 < TILES // 2)
        def _():
            for slot in range(2):
                start(down_copies(0, 2 * p + 2 + slot, slot))

        return 0

    lax.fori_loop(0, TILES // 2, forward, 0)
    start(weight_copies(1, 0, 0))
    copy(dy_hbm, dy, in_sem.at[1]).wait()
    for r in range(0, T, ROWS):
        rows = pl.ds(r, ROWS)
        state = h[rows] + acc[rows].astype(BF16)
        h[rows] = state
        wide = state.astype(F32)
        a[rows] = (wide * norm_scale(wide)).astype(BF16)
        acc[rows] = jnp.zeros((ROWS, D), F32)
    wait(save_copies(TILES - 2, 0))
    wait(save_copies(TILES - 1, 1))

    def products(g, states, hidden):
        slot = g % OUT_SLOTS
        down = dot(hidden, dy[...], (0, 0)).astype(BF16)
        for i in range(2):
            out_d[slot, i] = down[i * LANES : (i + 1) * LANES]
        both = dot(states[...], dgu[...], (0, 0)).astype(BF16)
        for q in range(4):
            out_gu[slot, q // 2, q % 2] = both[q * QD : (q + 1) * QD]
        start(near_copies(g))

    def second(g, _):
        slot = g % 2
        wait(weight_copies(1, g, slot))

        @pl.when(g + 1 < TILES)
        def _():
            start(weight_copies(1, g + 1, 1 - slot))

        for r in range(0, T, ROWS):
            rows = pl.ds(r, ROWS)
            both = dot(a[rows], w[slot], (1, 0))
            gate, up = both[:, :TILE], both[:, TILE:]
            by_hidden = dot(dy[rows], wd[pl.ds(pl.multiple_of(slot * TILE, TILE), TILE)], (1, 1)).astype(BF16).astype(F32)
            s = jax.nn.sigmoid(gate)
            silu = gate * s
            hid[0, rows] = (silu * up).astype(BF16)
            dgu[rows, :TILE] = (by_hidden * (up * (s + silu * (1.0 - s)))).astype(BF16)
            dgu[rows, TILE:] = (by_hidden * silu).astype(BF16)

        products(g, a, hid[0])
        for r in range(0, T, ROWS):
            rows = pl.ds(r, ROWS)
            acc[rows] += dot(dgu[rows], w[slot], (1, 1))

        @pl.when(g >= LAG)
        def _():
            collect(g - LAG)

        send_across(g)

        return 0

    lax.fori_loop(0, TILES, second, 0)
    start(weight_copies(0, 0, 0, False))
    start(load_copies(0, 0))
    for r in range(0, T, ROWS):
        rows = pl.ds(r, ROWS)
        wide = h[rows].astype(F32)
        scale = norm_scale(wide)
        by_a = acc[rows].astype(BF16).astype(F32)
        along = jnp.mean(by_a * wide, -1, keepdims=True)
        dy[rows] += (by_a * scale - wide * (scale * scale * scale * along)).astype(BF16)

    def first(t, _):
        g, slot = t + TILES, t % 2
        wait(weight_copies(0, t, slot, False))
        wait(load_copies(t, slot))

        @pl.when(t + 1 < TILES)
        def _():
            start(weight_copies(0, t + 1, 1 - slot, False))
            start(load_copies(t + 1, 1 - slot))

        for r in range(0, T, ROWS):
            rows = pl.ds(r, ROWS)
            by_hidden = dot(dy[rows], wd[pl.ds(pl.multiple_of(slot * TILE, TILE), TILE)], (1, 1)).astype(BF16).astype(F32)
            dgu[rows, :TILE] = (by_hidden * sr[slot, rows, :TILE]).astype(BF16)
            dgu[rows, TILE:] = (by_hidden * sr[slot, rows, TILE:]).astype(BF16)
        products(g, a0, hid[slot])
        collect(g - LAG)
        send_across(g)
        return 0

    lax.fori_loop(0, TILES, first, 0)
    last = LAYERS * TILES
    for g in range(last - LAG, last):
        collect(g)
    wait(gu_copies(last - 2) + gu_copies(last - 1))
    d_copy(last - 4 + chip).wait()
    d_copy(last - 2 + chip).wait()

    ss_all[me] = ss[...]
    sums = [
        remote(ss, ss_all.at[me], ss_send.at[i], ss_recv.at[me], lax.rem(me + 1 + i, 4)) for i in range(3)
    ]
    start(sums)
    for i in range(3):
        frm = lax.rem(me + 1 + i, 4)
        remote(ss, ss_all.at[frm], ss_send.at[i], ss_recv.at[frm], frm).wait()
    ss_out[...] = ss_all[0] + ss_all[1] + ss_all[2] + ss_all[3]


def gradients(x, dy, wg, wu, wd):
    hbm = pl.BlockSpec(memory_space=pl.ANY)
    vmem = pl.BlockSpec(memory_space=pltpu.VMEM)
    shape = jax.ShapeDtypeStruct
    tokens = pltpu.VMEM((T, D), BF16)
    dma = pltpu.SemaphoreType.DMA
    return pl.pallas_call(
        gradients_kernel,
        name="gradients",
        in_specs=[hbm] * 5,
        out_specs=[hbm] * 3 + [vmem] + [hbm] * 2,
        out_shape=[
            shape((LAYERS, QD, F), BF16),
            shape((LAYERS, QD, F), BF16),
            shape((LAYERS, QF, D), BF16),
            shape((8, LANES), F32),
            shape((TILES, T, 2 * TILE), F32),
            shape((TILES, T, TILE), BF16),
        ],
        scratch_shapes=[
            tokens, tokens, tokens, tokens,
            pltpu.VMEM((T, D), F32),
            pltpu.VMEM((2, D, 2 * TILE), BF16),
            pltpu.VMEM((2 * TILE, D), BF16),
            pltpu.VMEM((2, T, 2 * TILE), F32),
            pltpu.VMEM((2, T, TILE), BF16),
            pltpu.VMEM((T, 2 * TILE), BF16),
            pltpu.VMEM((OUT_SLOTS, 2, 2, QD, 2 * TILE), BF16),
            pltpu.VMEM((OUT_SLOTS, 2, LANES, D), BF16),
            pltpu.VMEM((OUT_SLOTS, 2, QD, 2 * TILE), BF16),
            pltpu.VMEM((OUT_SLOTS, LANES, D), BF16),
            pltpu.VMEM((FAR_SLOTS, QD, 2 * TILE), BF16),
            pltpu.VMEM((FAR_SLOTS, LANES, D), BF16),
            pltpu.VMEM((FAR_SLOTS, QD, 2 * TILE), BF16),
            pltpu.VMEM((FAR_SLOTS, LANES, D), BF16),
            pltpu.VMEM((2, QD, 2 * TILE), BF16),
            pltpu.VMEM((2, LANES, D), BF16),
            pltpu.VMEM((8, LANES), F32),
            pltpu.VMEM((4, 8, LANES), F32),
            dma((2,)), dma((2, 6)), dma((2, 2)),
            dma((OUT_SLOTS, 2)), dma((OUT_SLOTS, 2)), dma((FAR_SLOTS, 2)), dma((FAR_SLOTS, 2)),
            dma((2, 5)), dma((3,)), dma((4,)),
        ],
        compiler_params=pltpu.CompilerParams(collective_id=0, has_side_effects=True, vmem_limit_bytes=VMEM_LIMIT),
        cost_estimate=pl.CostEstimate(flops=15 * 2 * T * D * F, bytes_accessed=500_000_000, transcendentals=4 * T * F),
    )(x, dy, wg, wu, wd)


FIRST, MIDDLE, LAST = (1, 1, 2), (2, 2), (4, 1, 1)


def adamw_kernel(me_ref, squares, g, w, m, v, *refs):
    new_w, new_m, new_v = refs[-3:]
    total = jnp.sum(squares[...], keepdims=True)
    factor = jnp.minimum(1.0, 0.5 * lax.rsqrt(total / (LAYERS * 3 * D * F) + 1e-30))
    grad = g[0].astype(F32) * factor
    old = w[0].astype(F32)
    mm = 0.9 * m[0] + 0.1 * grad
    vv = 0.95 * v[0] + 0.05 * grad * grad
    new_m[0], new_v[0] = mm, vv
    new_w[...] = (old - 0.02 * (mm * lax.rsqrt(vv + 1e-8) + 0.1 * old)).astype(BF16)


def adamw(me, squares, g, w, m, v, so_far, layer, first, rows):
    _, n, c = g.shape
    step_rows = 32 if c == F else 128
    start = first // step_rows
    at = pl.BlockSpec((1, step_rows, c), lambda i, me: (layer, start + i, 0))
    hbm = pl.BlockSpec(memory_space=pl.ANY)
    own = pl.BlockSpec((1, step_rows, c), lambda i, me: (layer, me[0] * (n // step_rows) + start + i, 0))
    moment = jax.ShapeDtypeStruct(m.shape, F32)
    before = () if so_far is None else so_far
    return pl.pallas_call(
        adamw_kernel,
        name=f"adamw_{layer}_{first}",
        grid_spec=pltpu.PrefetchScalarGridSpec(
            num_scalar_prefetch=1,
            grid=(rows // step_rows,),
            in_specs=[pl.BlockSpec((8, LANES), lambda i, me: (0, 0)), at, own, at, at] + [hbm] * len(before),
            out_specs=[pl.BlockSpec((step_rows, c), lambda i, me: (i, 0)), at, at],
        ),
        out_shape=[jax.ShapeDtypeStruct((rows, c), BF16), moment, moment],
        input_output_aliases={6: 1, 7: 2} if before else {},
        cost_estimate=pl.CostEstimate(flops=60 * rows * c, bytes_accessed=22 * rows * c, transcendentals=rows * c),
    )(me, squares, g, w, m, v, *before)


def empty(shape):
    return pl.pallas_call(
        lambda out: None, name="empty", out_specs=pl.BlockSpec(memory_space=pl.ANY), out_shape=jax.ShapeDtypeStruct(shape, BF16)
    )()


def pieces():
    for i in range(3):
        for layer in range(LAYERS):
            parts = FIRST if (i, layer) == (0, 0) else LAST if (i, layer) == (2, LAYERS - 1) else MIDDLE
            rows, first = (QD, QD, QF)[i], 0
            for part in parts:
                yield i, layer, first, part * rows // sum(parts)
                first += part * rows // sum(parts)


def step(x, dy, wg, wu, wd, *moments):
    me = lax.axis_index("dp")
    weights = (wg, wu, wd)
    *grads, squares = gradients(x[0], dy[0], wg, wu, wd)[:4]
    outs = [empty(w.shape) for w in weights]
    so_far = [None] * 3
    at = jnp.reshape(me, (1,)).astype(jnp.int32)
    sent = []
    for i, layer, first, rows in pieces():
        block, *so_far[i] = adamw(
            at, squares, grads[i], weights[i], moments[i], moments[3 + i], so_far[i], layer, first, rows
        )
        sent.append((block, lax.ppermute(block, "dp", PAIR), lax.ppermute(block, "dp", CROSS)))
    last = 0
    for number, ((i, layer, first, rows), (block, near, far)) in enumerate(zip(pieces(), sent, strict=True)):
        n = weights[i].shape[1] // 4
        far, outs[last] = lax.optimization_barrier((far, outs[last]))
        if number == 1:
            far, so_far = lax.optimization_barrier((far, so_far))
        for part, q in ((block, me), (near, me ^ 1), (far, me ^ 2), (lax.ppermute(far, "dp", PAIR), me ^ 3)):
            outs[i] = lax.dynamic_update_slice(outs[i], part[None], (layer, q * n + first, 0))
        last = i
    return (*outs, *(s[0] for s in so_far), *(s[1] for s in so_far))


def solution(mesh):
    tokens = P(("rep", "dp"), None, None)
    whole, rows = P(None, None, None), P(None, "dp", None)
    return jax.shard_map(
        step,
        mesh=mesh,
        in_specs=(tokens,) * 2 + (whole,) * 3 + (rows,) * 6,
        out_specs=(P("rep", None, None),) * 3 + (P("rep", "dp", None),) * 6,
        check_vma=False,
    )
```

```python
import jax
import jax.numpy as jnp
from jax import lax
from jax.experimental import pallas as pl
from jax.experimental.pallas import tpu as pltpu
from jax.sharding import PartitionSpec as P

F32, BF16 = jnp.float32, jnp.bfloat16
LAYERS = 2
T, D, F = 2048, 1024, 6144
QD, QF = D // 4, F // 4
LANES = 128
TILE = 2 * LANES
TILES = F // TILE
ROWS = 256
SHARED = 512
LAG = 3
OUT_SLOTS, FAR_SLOTS = LAG + 2, 2 * LAG
CROSS = [(i, i ^ 2) for i in range(4)]
PAIR = [(i, i ^ 1) for i in range(4)]
VMEM_LIMIT = 64 * 1024 * 1024 - 65536


def dot(a, b, contract):
    return lax.dot_general(a, b, ((contract[:1], contract[1:]), ((), ())), preferred_element_type=F32)


def norm_scale(wide):
    return lax.rsqrt(jnp.mean(wide * wide, -1, keepdims=True) + 1e-6)


def hidden_tile(t):
    first = (t % 2) * (2 * QF) + (t // 2) * LANES
    return first, first + QF


def gradients_kernel(
    x_hbm, dy_hbm, wg_hbm, wu_hbm, wd_hbm, m_hbm, v_hbm,
    gg_hbm, gu_hbm, gd_hbm, ss_out, g_across, m_across, v_across, sr_hbm, hid_hbm,
    h, a, a0, dy, acc, w, wd, sr, hid, dgu,
    out_gu, out_d, near_gu, near_d, send_gu, send_d, far_gu, far_d, g_gu, g_d, ss, ss_all,
    in_sem, w_sem, save_sem, near_send, near_recv, far_send, far_recv, g_sem, ss_send, ss_recv, mv_send, mv_recv,
):
    me, rep = lax.axis_index("dp"), lax.axis_index("rep")
    chip, core = me // 2, me % 2
    partner = chip * 2 + (1 - core)
    across = (1 - chip) * 2 + core

    def copy(src, dst, sem):
        return pltpu.make_async_copy(src, dst, sem)

    def remote(src, dst, send, recv, to):
        return pltpu.make_async_remote_copy(
            src, dst, send, recv, device_id=(rep, to), device_id_type=pl.DeviceIdType.MESH
        )

    def down_copies(layer, t, slot):
        copies = []
        for i, first in enumerate(hidden_tile(t)):
            to = wd.at[pl.ds(pl.multiple_of(slot * TILE + i * LANES, LANES), LANES)]
            copies.append(copy(wd_hbm.at[layer, pl.ds(pl.multiple_of(first, LANES), LANES)], to, w_sem.at[slot, i]))
        return copies

    def gate_up_copies(layer, t, slot):
        copies = []
        for i, first in enumerate(hidden_tile(t)):
            for j, whole in enumerate((wg_hbm, wu_hbm)):
                to = w.at[slot, :, pl.ds(j * TILE + i * LANES, LANES)]
                src = whole.at[layer, :, pl.ds(pl.multiple_of(first, LANES), LANES)]
                copies.append(copy(src, to, w_sem.at[slot, 2 + 2 * j + i]))
        return copies

    def weight_copies(layer, t, slot, gate_up=True):
        return down_copies(layer, t, slot) + (gate_up_copies(layer, t, slot) if gate_up else [])

    def start(copies):
        for c in copies:
            c.start()

    def wait(copies):
        for c in copies:
            c.wait()

    def save_copies(t, slot):
        return [copy(sr.at[slot], sr_hbm.at[t], save_sem.at[slot, 0]), copy(hid.at[slot], hid_hbm.at[t], save_sem.at[slot, 1])]

    def load_copies(t, slot):
        return [copy(sr_hbm.at[t], sr.at[slot], save_sem.at[slot, 0]), copy(hid_hbm.at[t], hid.at[slot], save_sem.at[slot, 1])]

    def near_copies(g):
        slot = g % OUT_SLOTS
        return [
            remote(out_gu.at[slot, :, 1 - core], near_gu.at[slot], near_send.at[slot, 0], near_recv.at[slot, 0], partner),
            remote(out_d.at[slot, 1 - core], near_d.at[slot], near_send.at[slot, 1], near_recv.at[slot, 1], partner),
        ]

    def far_gu_copy(g):
        slot = g % FAR_SLOTS
        return remote(send_gu.at[slot], far_gu.at[slot], far_send.at[slot, 0], far_recv.at[slot, 0], across)

    def far_d_copy(g):
        slot = g % FAR_SLOTS
        return remote(send_d.at[slot], far_d.at[slot], far_send.at[slot, 1], far_recv.at[slot, 1], across)

    def moment_copies():
        return [
            remote(m_hbm.at[1, pl.ds(0, SHARED)], m_across, mv_send.at[0], mv_recv.at[0], across),
            remote(v_hbm.at[1, pl.ds(0, SHARED)], v_across, mv_send.at[1], mv_recv.at[1], across),
        ]

    def shared(g):
        return g < 2 * (SHARED // LANES)

    def send_across(g):
        slot, far = g % OUT_SLOTS, g % FAR_SLOTS
        wait(near_copies(g))
        send_gu[far] = (out_gu[slot, 1 - chip, core].astype(F32) + near_gu[slot, 1 - chip].astype(F32)).astype(BF16)
        far_gu_copy(g).start()

        @pl.when((g % 2 != chip) | shared(g))
        def _():
            send_d[far] = (out_d[slot, core].astype(F32) + near_d[slot].astype(F32)).astype(BF16)
            far_d_copy(g).start()

    def gu_copies(g):
        layer, t, slot = 1 - g // TILES, g % TILES, g % 2
        copies = []
        for i, first in enumerate(hidden_tile(t)):
            first = pl.multiple_of(first, LANES)
            for j, to in enumerate((gg_hbm, gu_hbm)):
                src = g_gu.at[slot, :, pl.ds(j * TILE + i * LANES, LANES)]
                copies.append(copy(src, to.at[layer, :, pl.ds(first, LANES)], g_sem.at[slot, 2 * j + i]))
        return copies

    def d_copy(g):
        layer, t, slot = 1 - g // TILES, g % TILES, g % 2
        return copy(g_d.at[slot], gd_hbm.at[layer, pl.ds(pl.multiple_of((t // 2) * LANES, LANES), LANES)], g_sem.at[slot, 4])

    def d_across_copy(g):
        slot = g % 2
        return copy(g_d.at[slot], g_across.at[pl.ds(pl.multiple_of((g // 2) * LANES, LANES), LANES)], g_sem.at[slot, 4])

    def add_squares(block):
        wide = block.astype(F32)
        wide = jnp.sum((wide * wide).reshape(-1, 8, wide.shape[1]), 0)
        ss[...] += sum(wide[:, i : i + LANES] for i in range(0, wide.shape[1], LANES))

    def collect(g):
        slot, far = g % OUT_SLOTS, g % FAR_SLOTS
        far_gu_copy(g).wait()

        @pl.when(g >= 2)
        def _():
            wait(gu_copies(g - 2))

        total = out_gu[slot, chip, core].astype(F32) + near_gu[slot, chip].astype(F32) + far_gu[far].astype(F32)
        g_gu[g % 2] = total.astype(BF16)
        start(gu_copies(g))
        add_squares(total.astype(BF16))

        @pl.when((g % 2 != chip) | shared(g))
        def _():
            far_d_copy(g).wait_send()

        @pl.when((g % 2 == chip) | shared(g))
        def _():
            far_d_copy(g).wait_recv()

        @pl.when(shared(g))
        def _():
            @pl.when(g >= 2)
            def _():
                @pl.when(g % 2 == chip)
                def _():
                    d_copy(g - 2).wait()

                @pl.when(g % 2 != chip)
                def _():
                    d_across_copy(g - 2).wait()

            total = (send_d[far].astype(F32) + far_d[far].astype(F32)).astype(BF16)
            g_d[g % 2] = total

            @pl.when(g % 2 == chip)
            def _():
                d_copy(g).start()
                add_squares(total)

            @pl.when(g % 2 != chip)
            def _():
                d_across_copy(g).start()

        @pl.when((g % 2 == chip) & jnp.logical_not(shared(g)))
        def _():
            d_copy(g - 2).wait()
            total = out_d[slot, core].astype(F32) + near_d[slot].astype(F32) + far_d[far].astype(F32)
            g_d[g % 2] = total.astype(BF16)
            d_copy(g).start()
            add_squares(total.astype(BF16))

    for slot in range(2):
        start(weight_copies(0, slot, slot))
    start([copy(x_hbm, h, in_sem.at[0]), copy(dy_hbm, dy, in_sem.at[1])])
    barrier = pltpu.get_barrier_semaphore()
    for other in range(1, 4):
        pl.semaphore_signal(barrier, inc=1, device_id=(rep, lax.rem(me + other, 4)), device_id_type=pl.DeviceIdType.MESH)
    pl.semaphore_wait(barrier, 3)
    start(moment_copies())
    ss[...] = jnp.zeros_like(ss)

    def by_rows(do):
        def some(r, _):
            do(pl.ds(pl.multiple_of(r * ROWS, ROWS), ROWS))
            return 0

        lax.fori_loop(0, T // ROWS, some, 0)

    def clear(rows):
        acc[rows] = jnp.zeros((ROWS, D), F32)

    def norm_first(rows):
        wide = h[rows].astype(F32)
        a0[rows] = (wide * norm_scale(wide)).astype(BF16)

    by_rows(clear)
    copy(x_hbm, h, in_sem.at[0]).wait()
    by_rows(norm_first)

    def forward(p, _):
        for slot in range(2):
            t = 2 * p + slot
            wait(gate_up_copies(0, t, slot))

            @pl.when(p >= 1)
            def _():
                wait(save_copies(t - 2, slot))

            for r in range(0, T, ROWS):
                rows = pl.ds(r, ROWS)
                both = dot(a0[rows], w[slot], (1, 0))
                gate, up = both[:, :TILE], both[:, TILE:]
                s = jax.nn.sigmoid(gate)
                silu = gate * s
                sr[slot, rows, :TILE] = up * (s + silu * (1.0 - s))
                sr[slot, rows, TILE:] = silu
                hidden = (silu * up).astype(BF16)
                hid[slot, rows] = hidden
                dgu[rows, slot * TILE : (slot + 1) * TILE] = hidden
            start(save_copies(t, slot))

            @pl.when(p + 1 < TILES // 2)
            def _():
                start(gate_up_copies(0, t + 2, slot))

        for slot in range(2):
            wait(down_copies(0, 2 * p + slot, slot))
        for r in range(0, T, ROWS):
            rows = pl.ds(r, ROWS)
            acc[rows] += dot(dgu[rows], wd[...], (1, 0))

        @pl.when(p + 1 < TILES // 2)
        def _():
            for slot in range(2):
                start(down_copies(0, 2 * p + 2 + slot, slot))

        return 0

    lax.fori_loop(0, TILES // 2, forward, 0)
    start(weight_copies(1, 0, 0))
    copy(dy_hbm, dy, in_sem.at[1]).wait()

    def norm_second(rows):
        state = h[rows] + acc[rows].astype(BF16)
        h[rows] = state
        wide = state.astype(F32)
        a[rows] = (wide * norm_scale(wide)).astype(BF16)
        clear(rows)

    by_rows(norm_second)
    wait(save_copies(TILES - 2, 0))
    wait(save_copies(TILES - 1, 1))

    def products(g, states, hidden):
        slot = g % OUT_SLOTS
        down = dot(hidden, dy[...], (0, 0)).astype(BF16)
        for i in range(2):
            out_d[slot, i] = down[i * LANES : (i + 1) * LANES]
        both = dot(states[...], dgu[...], (0, 0)).astype(BF16)
        for q in range(4):
            out_gu[slot, q // 2, q % 2] = both[q * QD : (q + 1) * QD]
        start(near_copies(g))

    def second(g, _):
        slot = g % 2
        wait(weight_copies(1, g, slot))

        @pl.when(g + 1 < TILES)
        def _():
            start(weight_copies(1, g + 1, 1 - slot))

        for r in range(0, T, ROWS):
            rows = pl.ds(r, ROWS)
            both = dot(a[rows], w[slot], (1, 0))
            gate, up = both[:, :TILE], both[:, TILE:]
            by_hidden = dot(dy[rows], wd[pl.ds(pl.multiple_of(slot * TILE, TILE), TILE)], (1, 1)).astype(BF16).astype(F32)
            s = jax.nn.sigmoid(gate)
            silu = gate * s
            hid[0, rows] = (silu * up).astype(BF16)
            dgu[rows, :TILE] = (by_hidden * (up * (s + silu * (1.0 - s)))).astype(BF16)
            dgu[rows, TILE:] = (by_hidden * silu).astype(BF16)

        products(g, a, hid[0])
        for r in range(0, T, ROWS):
            rows = pl.ds(r, ROWS)
            acc[rows] += dot(dgu[rows], w[slot], (1, 1))

        @pl.when(g >= LAG)
        def _():
            collect(g - LAG)

        send_across(g)

        return 0

    lax.fori_loop(0, TILES, second, 0)
    start(weight_copies(0, 0, 0, False))
    start(load_copies(0, 0))

    def norm_back(rows):
        wide = h[rows].astype(F32)
        scale = norm_scale(wide)
        by_a = acc[rows].astype(BF16).astype(F32)
        along = jnp.mean(by_a * wide, -1, keepdims=True)
        dy[rows] += (by_a * scale - wide * (scale * scale * scale * along)).astype(BF16)

    by_rows(norm_back)

    def first(t, _):
        g, slot = t + TILES, t % 2
        wait(weight_copies(0, t, slot, False))
        wait(load_copies(t, slot))

        @pl.when(t + 1 < TILES)
        def _():
            start(weight_copies(0, t + 1, 1 - slot, False))
            start(load_copies(t + 1, 1 - slot))

        for r in range(0, T, ROWS):
            rows = pl.ds(r, ROWS)
            by_hidden = dot(dy[rows], wd[pl.ds(pl.multiple_of(slot * TILE, TILE), TILE)], (1, 1)).astype(BF16).astype(F32)
            dgu[rows, :TILE] = (by_hidden * sr[slot, rows, :TILE]).astype(BF16)
            dgu[rows, TILE:] = (by_hidden * sr[slot, rows, TILE:]).astype(BF16)
        products(g, a0, hid[slot])
        collect(g - LAG)
        send_across(g)
        return 0

    lax.fori_loop(0, TILES, first, 0)
    last = LAYERS * TILES

    def rest(g, _):
        collect(g)
        return 0

    lax.fori_loop(last - LAG, last, rest, 0)
    wait(gu_copies(last - 2) + gu_copies(last - 1))
    d_copy(last - 2 + chip).wait()
    d_across_copy(2 * (SHARED // LANES) - 1 - chip).wait()
    wait(moment_copies())

    ss_all[me] = ss[...]
    sums = [
        remote(ss, ss_all.at[me], ss_send.at[i], ss_recv.at[me], lax.rem(me + 1 + i, 4)) for i in range(3)
    ]
    start(sums)
    for i in range(3):
        frm = lax.rem(me + 1 + i, 4)
        remote(ss, ss_all.at[frm], ss_send.at[i], ss_recv.at[frm], frm).wait()
    ss_out[...] = ss_all[0] + ss_all[1] + ss_all[2] + ss_all[3]


def gradients(x, dy, wg, wu, wd, m, v):
    hbm = pl.BlockSpec(memory_space=pl.ANY)
    vmem = pl.BlockSpec(memory_space=pltpu.VMEM)
    shape = jax.ShapeDtypeStruct
    tokens = pltpu.VMEM((T, D), BF16)
    dma = pltpu.SemaphoreType.DMA
    return pl.pallas_call(
        gradients_kernel,
        name="gradients",
        in_specs=[hbm] * 7,
        out_specs=[hbm] * 3 + [vmem] + [hbm] * 5,
        out_shape=[
            shape((LAYERS, QD, F), BF16),
            shape((LAYERS, QD, F), BF16),
            shape((LAYERS, QF, D), BF16),
            shape((8, LANES), F32),
            shape((SHARED, D), BF16),
            shape((SHARED, D), F32),
            shape((SHARED, D), F32),
            shape((TILES, T, 2 * TILE), F32),
            shape((TILES, T, TILE), BF16),
        ],
        scratch_shapes=[
            tokens, tokens, tokens, tokens,
            pltpu.VMEM((T, D), F32),
            pltpu.VMEM((2, D, 2 * TILE), BF16),
            pltpu.VMEM((2 * TILE, D), BF16),
            pltpu.VMEM((2, T, 2 * TILE), F32),
            pltpu.VMEM((2, T, TILE), BF16),
            pltpu.VMEM((T, 2 * TILE), BF16),
            pltpu.VMEM((OUT_SLOTS, 2, 2, QD, 2 * TILE), BF16),
            pltpu.VMEM((OUT_SLOTS, 2, LANES, D), BF16),
            pltpu.VMEM((OUT_SLOTS, 2, QD, 2 * TILE), BF16),
            pltpu.VMEM((OUT_SLOTS, LANES, D), BF16),
            pltpu.VMEM((FAR_SLOTS, QD, 2 * TILE), BF16),
            pltpu.VMEM((FAR_SLOTS, LANES, D), BF16),
            pltpu.VMEM((FAR_SLOTS, QD, 2 * TILE), BF16),
            pltpu.VMEM((FAR_SLOTS, LANES, D), BF16),
            pltpu.VMEM((2, QD, 2 * TILE), BF16),
            pltpu.VMEM((2, LANES, D), BF16),
            pltpu.VMEM((8, LANES), F32),
            pltpu.VMEM((4, 8, LANES), F32),
            dma((2,)), dma((2, 6)), dma((2, 2)),
            dma((OUT_SLOTS, 2)), dma((OUT_SLOTS, 2)), dma((FAR_SLOTS, 2)), dma((FAR_SLOTS, 2)),
            dma((2, 5)), dma((3,)), dma((4,)), dma((2,)), dma((2,)),
        ],
        compiler_params=pltpu.CompilerParams(collective_id=0, has_side_effects=True, vmem_limit_bytes=VMEM_LIMIT),
        cost_estimate=pl.CostEstimate(flops=15 * 2 * T * D * F, bytes_accessed=500_000_000, transcendentals=4 * T * F),
    )(x, dy, wg, wu, wd, m, v)


BLOCK = (32, 1024)


def adamw_kernel(quarter, squares, g, w, m, v, *refs):
    new_w, new_m, new_v = refs[-3:]
    total = jnp.sum(squares[...], keepdims=True)
    factor = jnp.minimum(1.0, 0.5 * lax.rsqrt(total / (LAYERS * 3 * D * F) + 1e-30))
    across = g.shape[2] // BLOCK[1]

    def update(k, _):
        rows = pl.ds(pl.multiple_of((k // across) * BLOCK[0], BLOCK[0]), BLOCK[0])
        columns = pl.ds(pl.multiple_of((k % across) * BLOCK[1], BLOCK[1]), BLOCK[1])
        grad = g[0, rows, columns].astype(F32) * factor
        old = w[0, rows, columns].astype(F32)
        mm = 0.9 * m[0, rows, columns] + 0.1 * grad
        vv = 0.95 * v[0, rows, columns] + 0.05 * grad * grad
        new_m[0, rows, columns], new_v[0, rows, columns] = mm, vv
        new_w[rows, columns] = (old - 0.02 * (mm * lax.rsqrt(vv + 1e-8) + 0.1 * old)).astype(BF16)
        return 0

    lax.fori_loop(0, g.shape[1] // BLOCK[0] * across, update, 0)


def adamw(quarter, squares, g, w, m, v, so_far, layer, first, rows, w_layer):
    n, c = w.shape[1] // 4, w.shape[2]
    step_rows = 32 if c == F else 128
    start = first // step_rows
    at = pl.BlockSpec((1, step_rows, c), lambda i, q: (layer, start + i, 0))
    hbm = pl.BlockSpec(memory_space=pl.ANY)
    own = pl.BlockSpec((1, step_rows, c), lambda i, q: (w_layer, q[0] * (n // step_rows) + start + i, 0))
    moment = jax.ShapeDtypeStruct(m.shape, F32)
    before = () if so_far is None else so_far
    return pl.pallas_call(
        adamw_kernel,
        grid_spec=pltpu.PrefetchScalarGridSpec(
            num_scalar_prefetch=1,
            grid=(rows // step_rows,),
            in_specs=[pl.BlockSpec((8, LANES), lambda i, q: (0, 0)), at, own, at, at] + [hbm] * len(before),
            out_specs=[pl.BlockSpec((step_rows, c), lambda i, q: (i, 0)), at, at],
        ),
        out_shape=[jax.ShapeDtypeStruct((rows, c), BF16), moment, moment],
        input_output_aliases={6: 1, 7: 2} if before else {},
        cost_estimate=pl.CostEstimate(flops=60 * rows * c, bytes_accessed=22 * rows * c, transcendentals=rows * c),
    )(quarter, squares, g, w, m, v, *before)


def empty(shape):
    return pl.pallas_call(
        lambda out: None, name="empty", out_specs=pl.BlockSpec(memory_space=pl.ANY), out_shape=jax.ShapeDtypeStruct(shape, BF16)
    )()


def pieces():
    for i in range(3):
        for layer in range(LAYERS):
            rows = (128, 128) if i < 2 else (768, 768)
            if (i, layer) == (0, 0):
                rows = (32, 32, 64, 128)
            if (i, layer) == (2, 1):
                rows = (SHARED, 512, 256, 256)
            first = 0
            for number, some in enumerate(rows):
                yield i, layer, first, some, (i, layer, number) == (2, 1, 0)
                first += some


def step(x, dy, wg, wu, wd, *moments):
    me = lax.axis_index("dp")
    weights = (wg, wu, wd)
    *grads, squares, g_across, m_across, v_across = gradients(x[0], dy[0], wg, wu, wd, moments[2], moments[5])[:7]
    outs = [empty(w.shape) for w in weights]
    so_far = [None] * 3
    here, over = (jnp.reshape(q, (1,)).astype(jnp.int32) for q in (me, me ^ 2))
    sent = []
    for i, layer, first, rows, shared in pieces():
        block, *so_far[i] = adamw(
            here, squares, grads[i], weights[i], moments[i], moments[3 + i], so_far[i], layer, first, rows, layer
        )
        if shared:
            far = adamw(over, squares, g_across[None], wd, m_across[None], v_across[None], None, 0, 0, rows, layer)[0]
        else:
            far = lax.ppermute(block, "dp", CROSS)
        sent.append((block, lax.ppermute(block, "dp", PAIR), far))
    shared_number = next(k for k, piece in enumerate(pieces()) if piece[-1])
    last = 0
    for number, (i, layer, first, rows, _) in enumerate(pieces()):
        block, near, far = sent[number]
        n = weights[i].shape[1] // 4
        far, outs[last] = lax.optimization_barrier((far, outs[last]))
        if number == 2:
            shared_block, shared_near, shared_far = sent[shared_number]
            far, so_far, shared_far = lax.optimization_barrier((far, so_far, shared_far))
            sent[shared_number] = shared_block, shared_near, shared_far
        on = lax.ppermute(far, "dp", PAIR)
        for part, q in ((block, me), (near, me ^ 1), (far, me ^ 2), (on, me ^ 3)):
            outs[i] = lax.dynamic_update_slice(outs[i], part[None], (layer, q * n + first, 0))
        last = i
    return (*outs, *(s[0] for s in so_far), *(s[1] for s in so_far))


def solution(mesh):
    tokens = P(("rep", "dp"), None, None)
    whole, rows = P(None, None, None), P(None, "dp", None)
    return jax.shard_map(
        step,
        mesh=mesh,
        in_specs=(tokens,) * 2 + (whole,) * 3 + (rows,) * 6,
        out_specs=(P("rep", None, None),) * 3 + (P("rep", "dp", None),) * 6,
        check_vma=False,
    )
```
